32 devices in a mesh: section: 4 (over z), seq: 8 (over y, x, core).
Axes of the slice: x: 2, y: 2, z: 4, core: 2. Of those that a mesh axis runs over, the one named last changes fastest.
Arguments:
- saved: bfloat16 [4, 3, 1024, 2304], P('section', None, 'seq'), may hold values from -8 to 8
- cotangent: bfloat16 [3, 1024, 2304], P(None, 'seq'), may hold values from -0.109375 to 0.109375
- slot_table: int32 [4, 3], P('section'), may hold values from 0 to 2, each once within a row
- gain: float32 [4, 2304], P('section'), may hold values from 0.25 to 1.75
- value_weight: bfloat16 [4, 2304, 1024], P('section'), may hold values from -0.125 to 0.125
- out_weight: bfloat16 [4, 2304, 1024], P('section'), may hold values from -0.1875 to 0.1875
Outputs:
- value_grad: float32 [4, 2304, 1024], P('section', 'seq')
- out_grad: float32 [4, 2304, 1024], P('section', 'seq')
- gain_grad: float32 [4, 2304], P('section')
The draws below stay inside these ranges and needn't reach their ends.
Inputs may be any that keep to these rules, and one draw needn't show every extreme that they name: `slot_table`: each row names every stash slot once.
All inputs are finite; a program needn't handle non-finite values.
Results may differ from the reference program's by a relative error of at most 0.007.
Values may be sent and summed in bfloat16 or wider, within the bound.
No kernel may reach another device: no remote copies, remote signals or barrier semaphores. Data moves between devices by JAX's collectives and lax.ppermute only.
A program may use at most 128 MiB of HBM per device.

```python
import jax
import jax.numpy as jnp
from jax import lax

D = 2304
R = 1024
MICRO = 3
TOKENS = 1024
N_SECTION = 4


def strengthened(entries, own_key, source, target, shards_of, factor):
    owner, partner = [(jnp.arange(entries.shape[dim]) // (entries.shape[dim] // shards_of)).reshape([-1 if axis == dim else 1 for axis in range(entries.ndim)]) for dim in (source, target)]
    chosen = jax.random.permutation(own_key, shards_of)[partner]
    strong = (owner == chosen) | (owner == (partner + shards_of // 2) % shards_of)
    return jnp.where(strong, factor * entries, entries)


def block_scale(own_key, dims, pieces, low, high):
    loudness = 1.0
    for axis_at, shards_of in pieces:
        steps = jax.random.uniform(jax.random.fold_in(jax.random.fold_in(own_key, 6), axis_at), (shards_of,), jnp.float32, low / len(pieces), high / len(pieces))
        loudness = loudness * jnp.repeat(jnp.exp(steps), dims[axis_at] // shards_of).reshape((-1,) + (1,) * (len(dims) - 1 - axis_at))
    return loudness


def bell_draw(key, extent, spread, limit, shards=(), held_as=jnp.bfloat16):
    entries = spread * jax.random.normal(key, extent, jnp.float32)
    if shards:
        entries = entries * block_scale(key, extent, shards, -0.22, 0.18)
    return jnp.clip(entries, -limit, limit).astype(held_as)


def bell_draw_with(rng, extent, scale, most, shards, heavy, kind=jnp.bfloat16):
    drawn = scale * jax.random.normal(rng, extent, jnp.float32)
    if shards:
        drawn = drawn * block_scale(rng, extent, shards, -0.22, 0.18)
    return jnp.clip(strengthened(drawn, jax.random.fold_in(rng, 3), *heavy), -most, most).astype(kind)


def setup_inputs(seed: int = 0) -> dict:
    splits = jax.random.split(jax.random.key(seed), 7)
    return {
        "saved": bell_draw_with(splits[0], (N_SECTION, MICRO, TOKENS, D), 1.0, 8.0, ((0, 4), (2, 8)), (2, 3, 8, 2.0)),
        "cotangent": bell_draw(splits[1], (MICRO, TOKENS, D), ((MICRO * TOKENS) ** -0.5), 0.109375, ((1, 8),)),
        "slot_table": jax.vmap(lambda own: jax.random.permutation(own, MICRO))(jax.random.split(splits[2], N_SECTION)).reshape((N_SECTION, MICRO)).astype(jnp.int32),
        "gain": jnp.clip(1.0 + 0.15 * jax.random.normal(splits[3], (N_SECTION, D), jnp.float32), 0.25, 1.75),
        "value_weight": bell_draw(splits[4], (N_SECTION, D, R), D ** -0.5, 0.125, ((0, 4),)),
        "out_weight": bell_draw(splits[5], (N_SECTION, D, R), R ** -0.5, 0.1875, ((0, 4),)),
    }


EPSILON = 1e-06

def normalize(inputs, gain_row):
    value_rows = inputs.astype(jnp.float32)
    inv_rms = lax.rsqrt(lax.optimization_barrier(jnp.mean(value_rows * value_rows, axis=-1, keepdims=True)) + EPSILON)
    unit_rows = value_rows * inv_rms
    return (unit_rows, inv_rms, (unit_rows * gain_row).astype(jnp.bfloat16))

def layer_backward(inputs, grad_out, gain_row, w_value, w_out):
    unit_rows, inv_rms, normed = normalize(inputs, gain_row)
    value_out = jnp.dot(normed, w_value, preferred_element_type=jnp.float32).astype(jnp.bfloat16)
    grad_value = jnp.dot(grad_out, w_out, preferred_element_type=jnp.float32).astype(jnp.bfloat16)
    grad_normed = lax.dot_general(grad_value, w_value, (((1,), (1,)), ((), ())), preferred_element_type=jnp.float32)
    gain_term = lax.optimization_barrier(jnp.sum(grad_normed * unit_rows, axis=0))
    grad_unit = grad_normed * gain_row
    grad_in = grad_out.astype(jnp.float32) + inv_rms * (grad_unit - unit_rows * lax.optimization_barrier(jnp.mean(grad_unit * unit_rows, axis=-1, keepdims=True)))
    value_term = lax.dot_general(normed, grad_value, (((0,), (0,)), ((), ())), preferred_element_type=jnp.float32)
    out_term = lax.dot_general(grad_out, value_out, (((0,), (0,)), ((), ())), preferred_element_type=jnp.float32)
    return (grad_in.astype(jnp.bfloat16), gain_term, value_term, out_term)

def reference(saved, cotangent, slot_table, gain, value_weight, out_weight):
    grads = [cotangent[micro_index] for micro_index in range(MICRO)]
    value_list = []
    out_list = []
    gain_list = []
    for section_index in reversed(range(N_SECTION)):
        value_acc = jnp.zeros((D, R), jnp.float32)
        out_acc = jnp.zeros((D, R), jnp.float32)
        gain_acc = jnp.zeros((D,), jnp.float32)
        next_grads = []
        for micro_index in range(MICRO):
            slot_index = slot_table[section_index, micro_index].astype(jnp.int32)
            inputs = lax.dynamic_index_in_dim(saved[section_index], slot_index, 0, keepdims=False)
            grad_in, gain_term, value_term, out_term = layer_backward(inputs, grads[micro_index], gain[section_index], value_weight[section_index], out_weight[section_index])
            value_acc = value_acc + value_term
            out_acc = out_acc + out_term
            gain_acc = gain_acc + gain_term
            next_grads.append(grad_in)
        grads = next_grads
        value_list.insert(0, value_acc)
        out_list.insert(0, out_acc)
        gain_list.insert(0, gain_acc)
    return (jnp.stack(value_list), jnp.stack(out_list), jnp.stack(gain_list))
```

```python
import jax
import jax.numpy as jnp
from jax import lax
from jax.sharding import PartitionSpec as P

EPSILON = 1e-06
LAG = 2
CHUNKS = 8


def passed_along(value, axis, steps):
    count = lax.axis_size(axis)
    first, last = (max(0, -steps), min(count, count - steps))
    return lax.ppermute(value, axis, [(source, source + steps) for source in range(first, last)])


def swapped(value, axis, mask):
    count = lax.axis_size(axis)
    return lax.ppermute(value, axis, [(source, source ^ mask) for source in range(count)])


def reduced(first, second, summed, axis):
    count = lax.axis_size(axis)
    index = lax.axis_index(axis)
    bits = count.bit_length() - 1
    orders = (list(range(bits)), [0] + list(range(bits))[:0:-1])
    helds = [part.reshape((2,) * bits + (part.shape[0] // count, part.shape[1])) for part in (first, second)]
    lefts = [list(range(bits))[::-1] for _ in helds]
    for stage in range(bits):
        keeps = []
        gots = []
        for which in range(2):
            bit = orders[which][stage]
            at = lefts[which].index(bit)
            mine = (index >> bit) & 1
            keeps.append(lax.dynamic_index_in_dim(helds[which], mine, at, keepdims=False))
            give = lax.dynamic_index_in_dim(helds[which], 1 - mine, at, keepdims=False)
            gots.append(swapped(give.astype(jnp.bfloat16), axis, 1 << bit))
            lefts[which].remove(bit)
        got_sum = swapped(summed, axis, 1 << stage)
        gots[1], got_sum = lax.optimization_barrier((gots[1], got_sum))
        helds = [keep + got.astype(jnp.float32) for keep, got in zip(keeps, gots)]
        summed = summed + got_sum
    return (helds[0], helds[1], summed)


def per_device(saved, cotangent, slot_table, gain, value_weight, out_weight):
    section_count = lax.axis_size("section")
    section_index = lax.axis_index("section")
    micro_count = slot_table.shape[1]
    gain_row = gain[0]
    w_value = value_weight[0]
    w_out = out_weight[0]
    token_rows = cotangent.shape[1]
    width = w_value.shape[0]
    inner = w_value.shape[1]
    total = micro_count * token_rows
    chunks = CHUNKS
    piece = total // chunks

    ordered = jnp.take(saved[0], slot_table[0], axis=0, mode="clip").reshape(total, width)
    top = cotangent.reshape(total, width)
    rows_f32 = ordered.astype(jnp.float32)
    inv_all = lax.rsqrt(jnp.mean(rows_f32 * rows_f32, axis=-1, keepdims=True) + EPSILON)
    normed_all = (rows_f32 * inv_all * gain_row).astype(jnp.bfloat16)
    values_all = jnp.dot(normed_all, w_value, preferred_element_type=jnp.float32).astype(
        jnp.bfloat16
    )

    slots = chunks + LAG * (section_count - 1)
    delay = LAG * (section_count - 1 - section_index)
    is_last = section_index == section_count - 1
    nothing = jnp.zeros((piece, width), jnp.bfloat16)
    sent = []
    outgoing = []
    outs = []
    grad_values = []
    gain_acc = jnp.zeros((width,), jnp.float32)
    for slot in range(slots):
        top_piece = top[slot * piece : (slot + 1) * piece] if slot < chunks else nothing
        incoming = sent[slot - LAG] if slot >= LAG else nothing
        if slot > LAG:
            incoming, outgoing[-1] = lax.optimization_barrier((incoming, outgoing[-1]))
        grad_out = jnp.where(is_last, top_piece, incoming)
        chunk = jnp.clip(slot - delay, 0, chunks - 1)
        inputs = lax.dynamic_slice_in_dim(ordered, chunk * piece, piece, 0)
        inv_rms = lax.dynamic_slice_in_dim(inv_all, chunk * piece, piece, 0)
        unit_rows = inputs.astype(jnp.float32) * inv_rms
        grad_value = jnp.dot(grad_out, w_out, preferred_element_type=jnp.float32).astype(
            jnp.bfloat16
        )
        grad_normed = lax.dot_general(
            grad_value, w_value, (((1,), (1,)), ((), ())), preferred_element_type=jnp.float32
        )
        gain_acc = gain_acc + jnp.sum(grad_normed * unit_rows, axis=0)
        outs.append(grad_out)
        grad_values.append(grad_value)
        if slot + LAG < slots:
            grad_unit = grad_normed * gain_row
            grad_in = grad_out.astype(jnp.float32) + inv_rms * (
                grad_unit - unit_rows * jnp.mean(grad_unit * unit_rows, axis=-1, keepdims=True)
            )
            outgoing.append(grad_in.astype(jnp.bfloat16))
            sent.append(passed_along(outgoing[-1], "section", -1))
        else:
            outgoing.append(grad_value)
    grads_all = lax.dynamic_slice_in_dim(jnp.concatenate(outs, 0), delay * piece, total, 0)
    grad_values_all = lax.dynamic_slice_in_dim(
        jnp.concatenate(grad_values, 0), delay * piece, total, 0
    )
    value_acc = lax.dot_general(
        normed_all, grad_values_all, (((0,), (0,)), ((), ())), preferred_element_type=jnp.float32
    )
    out_acc = lax.dot_general(
        grads_all, values_all, (((0,), (0,)), ((), ())), preferred_element_type=jnp.float32
    )
    value_grad, out_grad, gain_total = reduced(value_acc, out_acc, gain_acc, "seq")
    return (value_grad[None], out_grad[None], gain_total[None])


def solution(mesh):
    in_specs = (
        P("section", None, "seq", None),
        P(None, "seq", None),
        P("section", None),
        P("section", None),
        P("section", None, None),
        P("section", None, None),
    )
    out_specs = (P("section", "seq", None), P("section", "seq", None), P("section", None))
    return jax.shard_map(
        per_device, mesh=mesh, in_specs=in_specs, out_specs=out_specs, check_vma=False
    )
```
